32 devices in a mesh: by: 4 (over z), bx: 8 (over y, x, core).
Axes of the slice: x: 2, y: 2, z: 4, core: 2. Of those that a mesh axis runs over, the one named last changes fastest.
Arguments:
- wave_fn: float32 [2048, 3, 3, 2048], P('bx', None, None, 'by')
- left_env: float32 [2048, 5, 2048], P('bx')
- mpo_ten: float32 [5, 3, 3, 5], replicated
- right_env: float32 [2048, 5, 2048], P('by')
Outputs:
- output: float32 [2048, 3, 3, 2048], P('bx', None, None, 'by')
All inputs are finite; a program needn't handle non-finite values.
Results may differ from the reference program's by a relative error of at most 0.001.
Values sent between devices are 32-bit elements.
A program may use at most 1 GiB of HBM per device.

```python
import jax
import jax.numpy as jnp
from jax import lax

BOND_DIM = 2048
PHYS_DIM = 3
MPO_DIM = 5


def setup_inputs(seed: int = 0) -> dict:
    key = jax.random.key(seed)
    k_wave, k_left, k_mpo, k_right = jax.random.split(key, 4)
    wave_fn = jax.random.normal(k_wave, (BOND_DIM, PHYS_DIM, PHYS_DIM, BOND_DIM), jnp.float32)
    left_env = jax.random.normal(k_left, (BOND_DIM, MPO_DIM, BOND_DIM), jnp.float32) * (BOND_DIM ** -0.5)
    mpo_ten = jax.random.normal(k_mpo, (MPO_DIM, PHYS_DIM, PHYS_DIM, MPO_DIM), jnp.float32) * ((MPO_DIM * PHYS_DIM) ** -0.5)
    right_env = jax.random.normal(k_right, (BOND_DIM, MPO_DIM, BOND_DIM), jnp.float32) * ((MPO_DIM * BOND_DIM) ** -0.5)
    return {'wave_fn': wave_fn, 'left_env': left_env, 'mpo_ten': mpo_ten, 'right_env': right_env}


def reference(wave_fn, left_env, mpo_ten, right_env):
    row_block = min(BOND_DIM, 128)
    block_count = BOND_DIM // row_block
    left_blocks = left_env.reshape(block_count, row_block, MPO_DIM, BOND_DIM)

    def one_block(left_rows):
        stage_one = jnp.einsum('auc,cpqf->aupqf', left_rows.astype(jnp.float32), wave_fn.astype(jnp.float32))
        stage_two = jnp.einsum('aupqf,uspv->asvqf', stage_one, mpo_ten.astype(jnp.float32))
        stage_three = jnp.einsum('asvqf,vtqr->astrf', stage_two, mpo_ten.astype(jnp.float32))
        return jnp.einsum('astrf,brf->astb', stage_three, right_env.astype(jnp.float32))

    out_blocks = lax.map(one_block, left_blocks)
    return out_blocks.reshape(BOND_DIM, PHYS_DIM, PHYS_DIM, BOND_DIM)
```

```python
import functools

import jax
import jax.numpy as jnp
from jax import lax
from jax.experimental import pallas as pl
from jax.experimental.pallas import tpu as pltpu
from jax.sharding import PartitionSpec as P

HIGH = lax.Precision.HIGHEST
C_CHUNKS = (64, 72, 56, 32, 32)
A_CHUNKS = (40, 48, 56, 56, 56)
W_ROWS = 8


def mpo_kernel(phys, mpo, splat_ref, src_ref, dst_ref, mid_ref):
    rows, cols = src_ref.shape[-2:]
    col_tiles = cols // 128

    def one_tile(step, carry):
        row = pl.multiple_of((step // col_tiles) * 8, 8)
        col = pl.multiple_of((step % col_tiles) * 128, 128)
        tile = (pl.ds(row, 8), pl.ds(col, 128))
        src = [[[src_ref[p * phys + q, r, *tile] for p in range(phys)] for r in range(mpo)] for q in range(phys)]
        for v in range(mpo):
            for t in range(phys):
                acc = [None] * phys
                for q in range(phys):
                    for r in range(mpo):
                        weight = splat_ref[v, t, q, r]
                        for p in range(phys):
                            term = weight * src[q][r][p]
                            acc[p] = term if acc[p] is None else acc[p] + term
                for p in range(phys):
                    mid_ref[p, v, t] = acc[p]
        mid = [[[mid_ref[p, v, t] for t in range(phys)] for v in range(mpo)] for p in range(phys)]
        for u in range(mpo):
            for s in range(phys):
                acc = [None] * phys
                for p in range(phys):
                    for v in range(mpo):
                        weight = splat_ref[u, s, p, v]
                        for t in range(phys):
                            term = weight * mid[p][v][t]
                            acc[t] = term if acc[t] is None else acc[t] + term
                for t in range(phys):
                    dst_ref[u, s * phys + t, *tile] = acc[t]
        return carry

    lax.fori_loop(0, (rows // 8) * col_tiles, one_tile, 0)


def apply_mpo(splat, src, into, start):
    pq, mpo, rows, cols = src.shape
    phys = splat.shape[1]
    total, in_place = into
    tile = W_ROWS
    first = start // tile
    out_shape = jax.ShapeDtypeStruct((mpo, pq, total, cols), jnp.float32)
    in_specs = [
        pl.BlockSpec(splat.shape, lambda i: (0,) * 6),
        pl.BlockSpec((pq, mpo, tile, cols), lambda i: (0, 0, i, 0)),
    ]
    operands = [splat, src]
    aliases = {}
    body = functools.partial(mpo_kernel, phys, mpo)
    if in_place is not None:
        in_specs.append(pl.BlockSpec(memory_space=pl.ANY))
        operands.append(in_place)
        aliases = {2: 0}
        inner = body
        body = lambda splat_ref, src_ref, old_ref, dst_ref, mid_ref: inner(splat_ref, src_ref, dst_ref, mid_ref)
    return pl.pallas_call(
        body,
        grid=(rows // tile,),
        out_shape=out_shape,
        in_specs=in_specs,
        out_specs=pl.BlockSpec((mpo, pq, tile, cols), lambda i: (0, 0, first + i, 0)),
        scratch_shapes=[pltpu.VMEM((phys, mpo, phys, 8, 128), jnp.float32)],
        input_output_aliases=aliases,
        cost_estimate=pl.CostEstimate(flops=rows * cols * 2700, bytes_accessed=rows * cols * 360, transcendentals=0),
        compiler_params=pltpu.CompilerParams(vmem_limit_bytes=60 * 1024 * 1024),
        name="mpo",
    )(*operands)


def copy_kernel(src_ref, dst_ref):
    dst_ref[0] = src_ref[...]


def split_left(left, parts):
    mpo, rows, bond = left.shape
    share = bond // parts
    return pl.pallas_call(
        copy_kernel,
        grid=(parts, mpo),
        out_shape=jax.ShapeDtypeStruct((parts, mpo, rows, share), jnp.float32),
        in_specs=[pl.BlockSpec((1, rows, share), lambda j, u: (u, 0, j))],
        out_specs=pl.BlockSpec((1, 1, rows, share), lambda j, u: (j, u, 0, 0)),
        name="split_left",
    )(left)


def solution(mesh):
    cols_n = mesh.shape['by']
    rows_n = mesh.shape['bx']

    def local_apply(wave_blk, left_rows, mpo_ten, right_rows):
        row_share, mpo, _ = left_rows.shape
        phys = wave_blk.shape[1]
        col_share = wave_blk.shape[3]
        pq = phys * phys
        wave = wave_blk.transpose(1, 2, 0, 3).reshape(pq, row_share, col_share)
        left = split_left(left_rows.transpose(1, 0, 2), rows_n)
        left = lax.all_to_all(left, 'bx', 0, 0, tiled=True)
        right = right_rows.transpose(1, 0, 2).reshape(mpo, col_share, cols_n, col_share)
        right = right.transpose(2, 0, 1, 3)
        splat = jnp.broadcast_to(mpo_ten[..., None, None], mpo_ten.shape + (8, 128))

        starts = [sum(C_CHUNKS[:i]) for i in range(len(C_CHUNKS))]
        gathered = []
        for start, rows in zip(starts, C_CHUNKS):
            gathered.append(lax.all_gather(wave[:, start:start + rows], 'by', axis=0, tiled=False))

        mid = None
        for i, start in enumerate(starts):
            mixed = lax.dot_general(gathered[i], right, (((0, 3), (0, 3)), ((), ())), precision=HIGH, preferred_element_type=jnp.float32)
            mid = apply_mpo(splat, mixed.transpose(0, 2, 1, 3), (row_share, mid), start)

        outs = []
        done = 0
        for rows in A_CHUNKS:
            part = lax.dot_general(left[:, :, done:done + rows], mid, (((1, 3), (0, 2)), ((), ())), precision=HIGH, preferred_element_type=jnp.float32)
            part = part.transpose(2, 0, 1, 3).reshape(pq, rows_n * rows, col_share)
            outs.append(lax.psum_scatter(part, 'bx', scatter_dimension=1, tiled=True))
            done += rows
        out = jnp.concatenate(outs, axis=1)
        return out.reshape(phys, phys, row_share, col_share).transpose(2, 0, 1, 3)

    return jax.shard_map(local_apply, mesh=mesh, in_specs=(P('bx', None, None, 'by'), P('bx', None, None), P(), P('by', None, None)), out_specs=P('bx', None, None, 'by'), check_vma=False)
```
